32 devices in a mesh: batch: 1 (over z), row: 4 (over y), col: 8 (over x, core).
Axes of the slice: x: 4, y: 4, z: 1, core: 2. Of those that a mesh axis runs over, the one named last changes fastest.
The devices are a block of a 4x4x8 slice.
Arguments:
- l_mat: bfloat16 [8192, 8192], P(('batch', 'row'), 'col')
- b_mat: bfloat16 [8192, 16384], P(('batch', 'row'), 'col')
Outputs:
- output: bfloat16 [8192, 16384], P(('batch', 'row'), 'col')
All inputs are finite; a program needn't handle non-finite values.
Results may differ from the reference program's by a relative error of at most 0.001.
Values are sent between devices in bfloat16 or wider.
A program may use at most 768 MiB of HBM per device.

```python
import jax
import jax.numpy as jnp

N = 8192
M = 16384


def setup_inputs(seed: int = 0, part: int = 0) -> dict:
    base_key = jax.random.fold_in(jax.random.key(seed), part)
    key_l, key_b = jax.random.split(base_key)
    row_scale = 1.0 / jnp.sqrt(jnp.arange(N, dtype=jnp.float32) + 1.0)
    l_full = jax.random.normal(key_l, (N, N), jnp.float32)
    l_mat = jnp.tril(l_full) * row_scale[:, None]
    b_mat = jax.random.normal(key_b, (N, M), jnp.float32)
    return {'l_mat': l_mat.astype(jnp.bfloat16), 'b_mat': b_mat.astype(jnp.bfloat16)}


def reference(l_mat, b_mat):
    product = jnp.dot(l_mat, b_mat, preferred_element_type=jnp.float32)
    return product.astype(jnp.bfloat16)
```

```python
import functools

import jax
import jax.numpy as jnp
from jax import lax
from jax.experimental import pallas as pl
from jax.experimental.pallas import tpu as pltpu
from jax.sharding import PartitionSpec as P

MESH = pl.DeviceIdType.MESH
CHUNKS = 4
TILES = 8
SLOTS = 2

ORDERS = (
    "00 01 10 11 02 12 03 13 04 14 20 21 22 23 24 05 15 25 06 16 26 30 31 32 33 34 35 36 07 17 27 37",
    "00 01 10 11 02 12 03 13 20 21 22 23 04 14 24 05 15 25 30 31 32 33 34 35 06 16 26 36 07 17 27 37",
    "00 01 02 03 10 11 12 13 20 21 22 23 04 14 24 30 31 32 33 34 05 15 25 35 06 16 26 36 07 17 27 37",
)
FORWARD_AT = (0, 0, 3, 5, 8, 14, 18, 23)
EXTRA, LOAD_B, FRESH_B, LOAD_L = 32, 64, 128, 256


def codes(order):
    tiles = [(0, int(t[0]), int(t[1])) for t in order.split()]
    tiles += [(1, i, j) for i in range(CHUNKS) for j in range(TILES)]
    out = []
    for n, (extra, i, j) in enumerate(tiles):
        code = i * TILES + j + EXTRA * extra
        if n == 0 or tiles[n - 1][2] != j or tiles[n - 1][0] != extra:
            code += LOAD_B
        if (extra, j) not in [(e, b) for e, _, b in tiles[:n]]:
            code += FRESH_B
        if (extra, i) not in [(e, a) for e, a, _ in tiles[:n]]:
            code += LOAD_L
        out.append(code)
    return out


def kernel(nrow, nx, l_ref, b_ref, x_ref, bg, lb, lv, bv, ov, acc,
           br, bs, bs2, gr, wr, ls, ps, ly, inj, lvs, bvs, xs, xr):
    rows, width = l_ref.shape
    cols = b_ref.shape[1]
    rc, half, tw = rows // CHUNKS, rows // CHUNKS // 2, cols // TILES

    row, col = lax.axis_index("row"), lax.axis_index("col")
    x, core = col // 2, col % 2
    right, left = (x + 1) % nx, (x + nx - 1) % nx
    up, down = (row + nrow - 1) % nrow, (row + 1) % nrow
    low = row < 2
    mirror = nrow - 1 - row
    wcore = jnp.where(low, 1, 0)
    gcore = 1 - wcore
    pmain = jnp.where(low, mirror, row)
    is_w, is_g = core == wcore, core == gcore
    low_w, low_g = jnp.logical_and(low, is_w), jnp.logical_and(low, is_g)
    high_w, high_g = jnp.logical_and(~low, is_w), jnp.logical_and(~low, is_g)

    def both(*conditions):
        return functools.reduce(jnp.logical_and, conditions)

    def needed(p, c, i):
        return jnp.logical_or(c <= 2 * p, jnp.logical_and(c == 2 * p + 1, i >= CHUNKS // 2))

    def device(r, xx, k):
        return {"row": r, "col": xx * 2 + k}

    partner = device(row, x, 1 - core)

    def remote(src, dst, send, recv, to):
        return pltpu.make_async_remote_copy(
            src_ref=src, dst_ref=dst, send_sem=send, recv_sem=recv, device_id=to, device_id_type=MESH)

    def arrived(ref, sem):
        pltpu.make_async_copy(ref, ref, sem).wait()

    def sent(ref, sem):
        pltpu.make_async_copy(ref, ref, sem).wait()

    def each(n, body):
        lax.fori_loop(0, n, lambda k, carry: (body(k), carry)[1], 0)

    barrier = pltpu.get_barrier_semaphore()
    peers = [partner] + [device(r, xx, k) for k in (0, 1)
                         for r, xx in ((row, right), (row, left), (up, x), (down, x))]
    for peer in peers:
        pl.semaphore_signal(barrier, inc=1, device_id=peer, device_id_type=MESH)
    pl.semaphore_wait(barrier, len(peers))

    def lrows(i):
        return pl.ds(pl.multiple_of(i * rc, rc), rc)

    def lhalf(i, d):
        return pl.ds(pl.multiple_of(i * rc + d * half, half), half)

    def bcols(j):
        return pl.ds(pl.multiple_of(j * tw, tw), tw)

    def gpiece(m, c, i, d):
        return lb.at[m, c, lhalf(i, d), :]

    def wpiece(m, c, i):
        return lb.at[m, c, lrows(i), :]

    def l_to_mirror(i):
        return remote(l_ref.at[lrows(i), :], wpiece(0, col, i), ly.at[i], gr.at[0, i, col, 0], device(mirror, x, 0))

    def l_own(m, i, d):
        return remote(l_ref.at[lhalf(i, d), :], gpiece(m, col, i, d), ls.at[m, i, col, d], gr.at[m, i, col, d],
                      device(row, right if d == 0 else left, gcore))

    def l_to_partner(m, i):
        return remote(l_ref.at[lrows(i), :], wpiece(m, col, i), ly.at[i], gr.at[m, i, col, 0], partner)

    first_row = jnp.where(core == 0,
                          jnp.where(row == 1, 2, 3),
                          jnp.where(row == 1, 0, jnp.where(row == 3, 0, 1)))

    def b_first(j):
        return remote(b_ref.at[:, bcols(j)], bg.at[row, :, bcols(j)], bs.at[j], br.at[row, j], device(first_row, x, core))

    def b_again(j):
        return remote(b_ref.at[:, bcols(j)], bg.at[0, :, bcols(j)], bs2.at[j], br.at[0, j], device(1, x, 0))

    fq = jnp.where(row == 3, 0, jnp.where(row == 2, 1, 2))
    ft = jnp.where(row == 3, 2, jnp.where(row == 2, 3, 0))
    forwards = jnp.logical_and(is_w, row > 0)

    def b_forward(j):
        ref = bg.at[fq, :, bcols(j)]
        return remote(ref, ref, bs2.at[j], br.at[fq, j], device(ft, x, core))

    def forward(j):
        arrived(bg.at[fq, :, bcols(j)], br.at[fq, j])
        b_forward(j).start()

    sends_b = ~both(row == 3, core == 0)
    g0 = both(row == 0, core == 0)
    w2 = both(row == 2, core == 0)

    def start_b(*js):
        for j in js:
            b_first(j).start()

    def start_l(i):
        @pl.when(needed(row, col, i))
        def _():
            l_to_mirror(i).start()

    @pl.when(is_w)
    def _():
        def go(i):
            @pl.when(needed(row, col, i))
            def _():
                m = jnp.where(low, 1, 0)
                l_own(m, i, 0).start()
                l_own(m, i, 1).start()

                @pl.when(low)
                def _():
                    l_to_partner(1, i).start()
        each(CHUNKS, go)

    @pl.when(high_w)
    def _():
        each(CHUNKS, start_l)

        def go(j):
            @pl.when(w2)
            def _():
                b_first(j).start()
            forward(j)
        each(TILES, go)

    @pl.when(both(high_g, row == 3))
    def _():
        start_l(0)
        start_l(1)
        start_b(0)
        start_l(2)
        start_b(1)
        start_l(3)
        start_b(*range(2, TILES))

    @pl.when(both(high_g, row == 2))
    def _():
        each(CHUNKS, start_l)
        each(TILES, lambda j: b_first(j).start())

    @pl.when(low)
    def _():
        each(TILES, lambda j: b_first(j).start())

    def product(a, k0, i, slot, p, t, deep):
        def dot(first, depth):
            lhs = lv[a, :, pl.ds(pl.multiple_of(k0 + first, rows), depth)]
            return jnp.dot(lhs, bv[slot, pl.ds(first, depth), :], preferred_element_type=jnp.float32)

        if deep:
            @pl.when(p >= 2)
            def _():
                acc[...] = dot(0, 2 * rows)
        for odd in (0, 1):
            for chunk in range(CHUNKS):
                depth = odd * rows + (chunk + 1) * rc

                @pl.when(both(p % 2 == odd, i == chunk))
                def _():
                    if deep:
                        last = dot(pl.multiple_of(p // 2 * (2 * rows), rows), depth)
                        ov[t] = (jnp.where(p >= 2, acc[...], 0.0) + last).astype(ov.dtype)
                    else:
                        ov[t] = dot(0, depth).astype(ov.dtype)

    def place(m, i):
        return jnp.where(m == 0, i, CHUNKS), jnp.where(m == 0, 0, i % 2 * (2 * rows))

    def copy_l(m, i, c, local):
        a, k0 = place(m, i)
        src = l_ref.at[lrows(i), :] if local else wpiece(m, c, i)
        to = lv.at[a, :, pl.ds(pl.multiple_of(k0 + c * width, width), width)]
        return pltpu.make_async_copy(src, to, lvs.at[c])

    def load_l(m, p, i, own, wait):
        def start(c):
            @pl.when(needed(p, c, i))
            def _():
                mine = jnp.logical_and(own, c == col)

                @pl.when(mine)
                def _():
                    copy_l(m, i, c, True).start()

                @pl.when(~mine)
                def _():
                    if wait:
                        arrived(wpiece(m, c, i), wr.at[m, i, c])
                    copy_l(m, i, c, False).start()
        each(2 * nx, start)

    def loaded_l(m, p, i):
        def finish(c):
            @pl.when(needed(p, c, i))
            def _():
                copy_l(m, i, c, True).wait()
        each(2 * nx, finish)

    def load_b(q, j, slot):
        def copy(local):
            src = b_ref.at[:, bcols(j)] if local else bg.at[q, :, bcols(j)]
            to = bv.at[slot, pl.ds(q * rows, rows), :]
            return pltpu.make_async_copy(src, to, bvs.at[slot, q])

        @pl.when(q == row)
        def _():
            copy(True).start()

        @pl.when(q != row)
        def _():
            copy(False).start()

    def loaded_b(q, slot):
        pltpu.make_async_copy(b_ref.at[:, bcols(0)], bv.at[slot, pl.ds(q * rows, rows), :], bvs.at[slot, q]).wait()

    def x_home(t, i, j):
        return remote(ov.at[t], x_ref.at[lrows(i), bcols(j)], xs.at[t], xr, device(mirror, x, core))

    def x_here(t, i, j):
        return pltpu.make_async_copy(ov.at[t], x_ref.at[lrows(i), bcols(j)], xs.at[t])

    def extra_rows(i):
        a, k0 = place(1, i)

        def start(j):
            for q in (0, 1):
                @pl.when(q <= row)
                def _():
                    @pl.when(jnp.logical_and(q != row, i == 0))
                    def _():
                        arrived(bg.at[q, :, bcols(j)], br.at[q, j])
                    load_b(q, j, j % SLOTS)

        load_l(1, row, i, True, False)
        start(0)
        loaded_l(1, row, i)

        def tile(j):
            for q in (0, 1):
                @pl.when(q <= row)
                def _():
                    loaded_b(q, j % SLOTS)

            @pl.when(j < TILES - 1)
            def _():
                start(j + 1)
            product(a, k0, i, j % SLOTS, row, i * TILES + j, False)
            x_here(i * TILES + j, i, j).start()
        each(TILES, tile)

    def hand(m, c, i, d):
        ref = gpiece(m, c, i, d)
        return remote(ref, ref, ps.at[m, i, c, d], wr.at[m, i, c], partner)

    def hand_own(m, i, d):
        return remote(l_ref.at[lhalf(i, d), :], gpiece(m, col, i, d), ps.at[m, i, col, d], wr.at[m, i, col], partner)

    def pass_on(m, c, i, d):
        ref = gpiece(m, c, i, d)
        return remote(ref, ref, ls.at[m, i, c, d], gr.at[m, i, c, d], device(row, right if d == 0 else left, gcore))

    steps = jnp.where(low, 2 * CHUNKS, CHUNKS)

    def stage(s, hop, drain):
        m, i = s // CHUNKS, s % CHUNKS
        p = jnp.where(m == 0, pmain, row)
        if hop == 0:
            foreign = jnp.logical_and(low, m == 0)

            @pl.when(foreign)
            def _():
                def go(e):
                    c = 2 * x + e

                    @pl.when(needed(p, c, i))
                    def _():
                        if not drain:
                            arrived(wpiece(m, c, i), gr.at[m, i, c, 0])
                        for d in (0, 1):
                            @pl.when(~both(row == 1, x == (nx - 2 if d == 0 else 0)))
                            def _():
                                copy = pass_on(m, c, i, d)
                                copy.wait_send() if drain else copy.start()
                            copy = hand(m, c, i, d)
                            copy.wait_send() if drain else copy.start()
                each(2, go)

            @pl.when(~foreign)
            def _():
                @pl.when(needed(p, col, i))
                def _():
                    for d in (0, 1):
                        for copy in (l_own(m, i, d), hand_own(m, i, d)):
                            copy.wait_send() if drain else copy.start()
                if not drain:
                    other = 2 * x + wcore

                    @pl.when(jnp.logical_and(low, needed(p, other, i)))
                    def _():
                        arrived(wpiece(m, other, i), gr.at[m, i, other, 0])
        else:
            def go(e):
                for d in (0, 1):
                    src = (x + nx - hop) % nx if d == 0 else (x + hop) % nx
                    c = 2 * src + e

                    @pl.when(needed(p, c, i))
                    def _():
                        if not drain:
                            arrived(gpiece(m, c, i, d), gr.at[m, i, c, d])
                        if hop < nx - 1:
                            copy = pass_on(m, c, i, d)
                            copy.wait_send() if drain else copy.start()
                        if hop == 1:
                            @pl.when(both(row == 2, x == nx - 1))
                            def _():
                                ref = gpiece(m, c, i, d)
                                copy = remote(ref, ref, inj.at[i, e, d], gr.at[m, i, c, d], device(1, x, 0))
                                copy.wait_send() if drain else copy.start()
                        copy = hand(m, c, i, d)
                        copy.wait_send() if drain else copy.start()
            each(2, go)

    @pl.when(is_g)
    def _():
        def wave(w):
            @pl.when(both(g0, w == nx - 1))
            def _():
                each(TILES, lambda j: b_again(j).start())
            for hop in reversed(range(nx)):
                s = w - hop

                @pl.when(jnp.logical_and(s >= 0, s < steps))
                def _():
                    stage(s, hop, False)

            done = w - (nx - 1)

            @pl.when(done >= CHUNKS)
            def _():
                extra_rows(done - CHUNKS)
        each(steps + nx - 1, wave)

        def drain(s):
            for hop in range(nx):
                stage(s, hop, True)
        each(steps, drain)

    count = CHUNKS * TILES

    def code_of(t):
        third = t // 3
        tables = [codes(order) for order in ORDERS]
        word = 0
        for n in range(0, len(tables[0]), 3):
            packed = [sum(v * 512**k for k, v in enumerate(table[n:n + 3])) for table in tables]
            at_row = jnp.where(row == 0, packed[0], jnp.where(row == 1, packed[1], packed[2]))
            word = jnp.where(third == n // 3, at_row, word)
        shift = jnp.where(t % 3 == 0, 1, jnp.where(t % 3 == 1, 512, 512 * 512))
        return word // shift % 512

    @pl.when(is_w)
    def _():
        total = jnp.where(low, 2 * count, count)

        def fields(code):
            m = code // EXTRA % 2
            return m, jnp.where(m == 1, row, pmain), code % EXTRA // TILES, code % TILES

        def flag(code, bit):
            return code // bit % 2 == 1

        def fetch(code, slot):
            m, p, i, j = fields(code)

            @pl.when(flag(code, LOAD_B))
            def _():
                for q in range(nrow):
                    @pl.when(q <= p)
                    def _():
                        known = jnp.logical_or(jnp.logical_and(forwards, q == fq), m == 1)

                        @pl.when(both(flag(code, FRESH_B), q != row, ~known))
                        def _():
                            arrived(bg.at[q, :, bcols(j)], br.at[q, j])
                        load_b(q, j, slot)

            @pl.when(flag(code, LOAD_L))
            def _():
                load_l(m, p, i, jnp.logical_or(m == 1, ~low), True)

        def step(t, carry):
            code, slot = carry
            m, p, i, j = fields(code)
            for j2, u2 in enumerate(FORWARD_AT):
                @pl.when(both(row == 1, t == u2))
                def _():
                    forward(j2)

            @pl.when(t == 0)
            def _():
                fetch(code, slot)

            @pl.when(flag(code, LOAD_B))
            def _():
                for q in range(nrow):
                    @pl.when(q <= p)
                    def _():
                        loaded_b(q, slot)

            @pl.when(flag(code, LOAD_L))
            def _():
                loaded_l(m, p, i)

            following = code_of(t + 1)
            other = jnp.where(flag(following, LOAD_B), 1 - slot, slot)

            @pl.when(t + 1 < total)
            def _():
                fetch(following, other)
            n = t % count

            @pl.when(t >= count)
            def _():
                sent(ov.at[n], xs.at[n])
            a, k0 = place(m, i)
            product(a, k0, i, slot, p, n, True)
            home = jnp.logical_and(low, m == 0)

            @pl.when(home)
            def _():
                x_home(n, i, j).start()

            @pl.when(~home)
            def _():
                x_here(n, i, j).start()
            return following, other
        lax.fori_loop(0, total, step, (code_of(0), 0))

    @pl.when(high_g)
    def _():
        arrived(x_ref, xr)

    @pl.when(jnp.logical_or(low, is_w))
    def _():
        each(count, lambda t: sent(ov.at[t], xs.at[t]))

    @pl.when(sends_b)
    def _():
        each(TILES, lambda j: b_first(j).wait_send())

    @pl.when(g0)
    def _():
        each(TILES, lambda j: b_again(j).wait_send())

    @pl.when(forwards)
    def _():
        each(TILES, lambda j: b_forward(j).wait_send())

    def drain(i):
        @pl.when(needed(row, col, i))
        def _():
            @pl.when(~low)
            def _():
                l_to_mirror(i).wait_send()

            @pl.when(is_w)
            def _():
                m = jnp.where(low, 1, 0)
                l_own(m, i, 0).wait_send()
                l_own(m, i, 1).wait_send()

            @pl.when(low_w)
            def _():
                l_to_partner(1, i).wait_send()
    each(CHUNKS, drain)


def solution(mesh):
    nrow, ncol = mesh.shape["row"], mesh.shape["col"]
    spec = P(("batch", "row"), "col")

    def local(l_block, b_block):
        rows, width = l_block.shape
        cols = b_block.shape[1]
        dtype = b_block.dtype
        rc, tw = rows // CHUNKS, cols // TILES
        dma = pltpu.SemaphoreType.DMA
        any_space = pl.BlockSpec(memory_space=pl.ANY)
        out = pl.pallas_call(
            functools.partial(kernel, nrow, ncol // 2),
            out_shape=(
                jax.ShapeDtypeStruct((rows, cols), dtype),
                jax.ShapeDtypeStruct((nrow, rows, cols), dtype),
                jax.ShapeDtypeStruct((2, ncol, rows, width), dtype),
            ),
            in_specs=[any_space] * 2,
            out_specs=(any_space,) * 3,
            scratch_shapes=[
                pltpu.VMEM((CHUNKS + 1, rc, ncol * width), dtype),
                pltpu.VMEM((SLOTS, nrow * rows, tw), dtype),
                pltpu.VMEM((CHUNKS * TILES, rc, tw), dtype),
                pltpu.VMEM((rc, tw), jnp.float32),
                dma((nrow, TILES)),
                dma((TILES,)),
                dma((TILES,)),
                dma((2, CHUNKS, ncol, 2)),
                dma((2, CHUNKS, ncol)),
                dma((2, CHUNKS, ncol, 2)),
                dma((2, CHUNKS, ncol, 2)),
                dma((CHUNKS,)),
                dma((CHUNKS, 2, 2)),
                dma((ncol,)),
                dma((SLOTS, nrow)),
                dma((CHUNKS * TILES,)),
                dma(()),
            ],
            compiler_params=pltpu.CompilerParams(collective_id=0, has_side_effects=True),
        )(l_block, b_block)
        return out[0]

    return jax.shard_map(local, mesh=mesh, in_specs=(spec, spec), out_specs=spec, check_vma=False)
```

```python
import functools

import jax
import jax.numpy as jnp
from jax import lax
from jax.experimental import pallas as pl
from jax.experimental.pallas import tpu as pltpu
from jax.sharding import PartitionSpec as P

MESH = pl.DeviceIdType.MESH
CHUNKS = 4
TILES = 8
SLOTS = 2

OWN = CHUNKS // 2
REST = " 24 23 22 21 20 05 15 25 06 16 26 07 17 27 37 36 35 34 33 32 31 30"
ORDERS = (
    " ".join(f"E0{j} E1{j}" for j in range(TILES)) + " 00 01 10 11 02 12 03 13 04 14" + REST,
    " ".join(f"E0{j}" for j in range(TILES)) + " 00 01 10 11 02 12 03 13 "
    + " ".join(f"E1{j}" for j in range(TILES)) + " 04 14" + REST,
    " ".join(["E00"] * OWN * TILES) + " 00 01 02 03 10 11 12 13 20 21 22 23 04 14 24 30 31 32 33 34"
    + " 05 15 25 35 06 16 26 36 07 17 27 37",
)
FORWARD_AT = (0, 7, 9, 11, 16, 23, 28, 33)
EXTRA, LOAD_B, FRESH_B, LOAD_L = 32, 64, 128, 256


def codes(order):
    tiles = [(len(t) - 2, int(t[-2]), int(t[-1])) for t in order.split()]
    out = []
    for n, (extra, i, j) in enumerate(tiles):
        code = i * TILES + j + EXTRA * extra
        if n == 0 or tiles[n - 1][2] != j or tiles[n - 1][0] != extra:
            code += LOAD_B
        if (extra, j) not in [(e, b) for e, _, b in tiles[:n]]:
            code += FRESH_B
        if (extra, i) not in [(e, a) for e, a, _ in tiles[:n]]:
            code += LOAD_L
        out.append(code)
    return out


def kernel(nrow, nx, l_ref, b_ref, x_ref, bg, lb, lv, bv, ov, acc,
           br, bs, bs2, gr, wr, ls, ps, ly, inj, lvs, bvs, xs, xr):
    rows, width = l_ref.shape
    cols = b_ref.shape[1]
    rc, half, tw = rows // CHUNKS, rows // CHUNKS // 2, cols // TILES

    row, col = lax.axis_index("row"), lax.axis_index("col")
    x, core = col // 2, col % 2
    right, left = (x + 1) % nx, (x + nx - 1) % nx
    up, down = (row + nrow - 1) % nrow, (row + 1) % nrow
    low = row < 2
    mirror = nrow - 1 - row
    wcore = jnp.where(low, 1, 0)
    gcore = 1 - wcore
    pmain = jnp.where(low, mirror, row)
    is_w, is_g = core == wcore, core == gcore
    low_w, low_g = jnp.logical_and(low, is_w), jnp.logical_and(low, is_g)
    high_w, high_g = jnp.logical_and(~low, is_w), jnp.logical_and(~low, is_g)

    def both(*conditions):
        return functools.reduce(jnp.logical_and, conditions)

    def needed(p, c, i):
        return jnp.logical_or(c <= 2 * p, jnp.logical_and(c == 2 * p + 1, i >= CHUNKS // 2))

    def device(r, xx, k):
        return {"row": r, "col": xx * 2 + k}

    partner = device(row, x, 1 - core)

    def remote(src, dst, send, recv, to):
        return pltpu.make_async_remote_copy(
            src_ref=src, dst_ref=dst, send_sem=send, recv_sem=recv, device_id=to, device_id_type=MESH)

    def arrived(ref, sem):
        pltpu.make_async_copy(ref, ref, sem).wait()

    def sent(ref, sem):
        pltpu.make_async_copy(ref, ref, sem).wait()

    def each(n, body):
        lax.fori_loop(0, n, lambda k, carry: (body(k), carry)[1], 0)

    barrier = pltpu.get_barrier_semaphore()
    peers = [partner] + [device(r, xx, k) for k in (0, 1)
                         for r, xx in ((row, right), (row, left), (up, x), (down, x))]
    for peer in peers:
        pl.semaphore_signal(barrier, inc=1, device_id=peer, device_id_type=MESH)
    pl.semaphore_wait(barrier, len(peers))

    def lrows(i):
        return pl.ds(pl.multiple_of(i * rc, rc), rc)

    def lhalf(i, d):
        return pl.ds(pl.multiple_of(i * rc + d * half, half), half)

    def bcols(j):
        return pl.ds(pl.multiple_of(j * tw, tw), tw)

    def gpiece(m, c, i, d):
        return lb.at[m, c, lhalf(i, d), :]

    def wpiece(m, c, i):
        return lb.at[m, c, lrows(i), :]

    def l_to_mirror(i):
        return remote(l_ref.at[lrows(i), :], wpiece(0, col, i), ly.at[i], gr.at[0, i, col, 0], device(mirror, x, 0))

    def l_own(m, i, d):
        return remote(l_ref.at[lhalf(i, d), :], gpiece(m, col, i, d), ls.at[m, i, col, d], gr.at[m, i, col, d],
                      device(row, right if d == 0 else left, gcore))

    def l_to_partner(m, i):
        return remote(l_ref.at[lrows(i), :], wpiece(m, col, i), ly.at[i], gr.at[m, i, col, 0], partner)

    first_row = jnp.where(core == 0,
                          jnp.where(row == 1, 2, 3),
                          jnp.where(row == 1, 0, jnp.where(row == 3, 0, 1)))

    def b_first(j):
        return remote(b_ref.at[:, bcols(j)], bg.at[row, :, bcols(j)], bs.at[j], br.at[row, j], device(first_row, x, core))

    def b_again(j):
        return remote(b_ref.at[:, bcols(j)], bg.at[0, :, bcols(j)], bs2.at[j], br.at[0, j], device(1, x, 0))

    fq = jnp.where(row == 3, 0, jnp.where(row == 2, 1, 2))
    ft = jnp.where(row == 3, 2, jnp.where(row == 2, 3, 0))
    forwards = jnp.logical_and(is_w, row > 0)

    def b_forward(j):
        ref = bg.at[fq, :, bcols(j)]
        return remote(ref, ref, bs2.at[j], br.at[fq, j], device(ft, x, core))

    def forward(j):
        arrived(bg.at[fq, :, bcols(j)], br.at[fq, j])
        b_forward(j).start()

    sends_b = ~both(row == 3, core == 0)
    g0 = both(row == 0, core == 0)
    w2 = both(row == 2, core == 0)
    last2 = both(row == 2, core == 1, x == nx - 1)

    def start_b(*js):
        for j in js:
            b_first(j).start()

    def start_l(i):
        @pl.when(needed(row, col, i))
        def _():
            l_to_mirror(i).start()

    @pl.when(is_w)
    def _():
        def go(i):
            @pl.when(needed(row, col, i))
            def _():
                m = jnp.where(low, 1, 0)
                l_own(m, i, 0).start()
                l_own(m, i, 1).start()

                @pl.when(low)
                def _():
                    l_to_partner(1, i).start()
        each(CHUNKS, go)

    @pl.when(high_w)
    def _():
        each(CHUNKS, start_l)

        def go(j):
            @pl.when(w2)
            def _():
                b_first(j).start()
            forward(j)
        each(TILES, go)

    @pl.when(jnp.logical_and(high_g, ~last2))
    def _():
        start_l(0)
        start_l(1)
        start_b(0)
        start_l(2)
        start_b(1)
        start_l(3)
        start_b(*range(2, TILES))

    @pl.when(low)
    def _():
        each(TILES, lambda j: b_first(j).start())

    def place(m, i):
        return jnp.where(m == 0, i, CHUNKS - 1), jnp.where(m == 0, 0, i * (2 * rows))

    def product(m, i, slot, p, t, deep):
        a, k0 = place(m, i)

        def dot(first, depth):
            lhs = lv[a, :, pl.ds(pl.multiple_of(k0 + first, rows), depth)]
            return jnp.dot(lhs, bv[slot, pl.ds(first, depth), :], preferred_element_type=jnp.float32)

        if deep:
            @pl.when(p >= 2)
            def _():
                acc[...] = dot(0, 2 * rows)
        for odd in (0, 1):
            for chunk in range(CHUNKS if deep else OWN):
                depth = odd * rows + (chunk + 1) * rc

                @pl.when(both(p % 2 == odd, i == chunk))
                def _():
                    if deep:
                        last = dot(pl.multiple_of(p // 2 * (2 * rows), rows), depth)
                        ov[t] = (jnp.where(p >= 2, acc[...], 0.0) + last).astype(ov.dtype)
                    else:
                        ov[t] = dot(0, depth).astype(ov.dtype)

    def copy_l(m, i, c, local):
        a, k0 = place(m, i)
        src = l_ref.at[lrows(i), :] if local else wpiece(m, c, i)
        to = lv.at[a, :, pl.ds(pl.multiple_of(k0 + c * width, width), width)]
        return pltpu.make_async_copy(src, to, lvs.at[i, c])

    def load_l(m, p, i, own, wait):
        def start(c):
            @pl.when(needed(p, c, i))
            def _():
                mine = jnp.logical_and(own, c == col)

                @pl.when(mine)
                def _():
                    copy_l(m, i, c, True).start()

                @pl.when(~mine)
                def _():
                    if wait:
                        arrived(wpiece(m, c, i), wr.at[m, i, c])
                    copy_l(m, i, c, False).start()
        each(2 * nx, start)

    def loaded_l(m, p, i):
        def finish(c):
            @pl.when(needed(p, c, i))
            def _():
                copy_l(m, i, c, True).wait()
        each(2 * nx, finish)

    def load_b(q, j, slot):
        def copy(local):
            src = b_ref.at[:, bcols(j)] if local else bg.at[q, :, bcols(j)]
            to = bv.at[slot, pl.ds(q * rows, rows), :]
            return pltpu.make_async_copy(src, to, bvs.at[slot, q])

        @pl.when(q == row)
        def _():
            copy(True).start()

        @pl.when(q != row)
        def _():
            copy(False).start()

    def loaded_b(q, slot):
        pltpu.make_async_copy(b_ref.at[:, bcols(0)], bv.at[slot, pl.ds(q * rows, rows), :], bvs.at[slot, q]).wait()

    def x_home(t, i, j):
        return remote(ov.at[t], x_ref.at[lrows(i), bcols(j)], xs.at[t], xr, device(mirror, x, core))

    def x_here(t, i, j):
        return pltpu.make_async_copy(ov.at[t], x_ref.at[lrows(i), bcols(j)], xs.at[t])

    def extra_rows(i):
        def start(j):
            for q in (0, 1):
                @pl.when(q <= row)
                def _():
                    @pl.when(jnp.logical_and(q != row, i == 0))
                    def _():
                        arrived(bg.at[q, :, bcols(j)], br.at[q, j])
                    load_b(q, j, j % SLOTS)

        load_l(1, row, i, True, False)
        start(0)
        loaded_l(1, row, i)

        def tile(j):
            for q in (0, 1):
                @pl.when(q <= row)
                def _():
                    loaded_b(q, j % SLOTS)

            @pl.when(j < TILES - 1)
            def _():
                start(j + 1)
            product(1, i, j % SLOTS, row, i * TILES + j, False)
            x_here(i * TILES + j, i, j).start()
        each(TILES, tile)

    def hand(m, c, i, d):
        ref = gpiece(m, c, i, d)
        return remote(ref, ref, ps.at[m, i, c, d], wr.at[m, i, c], partner)

    def hand_own(m, i, d):
        return remote(l_ref.at[lhalf(i, d), :], gpiece(m, col, i, d), ps.at[m, i, col, d], wr.at[m, i, col], partner)

    def pass_on(m, c, i, d):
        ref = gpiece(m, c, i, d)
        return remote(ref, ref, ls.at[m, i, c, d], gr.at[m, i, c, d], device(row, right if d == 0 else left, gcore))

    steps = jnp.where(low, 2 * CHUNKS, CHUNKS)

    def stage(s, hop, drain):
        m, i = jnp.where(low, s % 2, 0), jnp.where(low, s // 2, s)
        p = jnp.where(m == 0, pmain, row)
        if hop == 0:
            foreign = jnp.logical_and(low, m == 0)

            @pl.when(foreign)
            def _():
                def go(e):
                    c = 2 * x + e

                    @pl.when(needed(p, c, i))
                    def _():
                        if not drain:
                            arrived(wpiece(m, c, i), gr.at[m, i, c, 0])
                        for d in (0, 1):
                            @pl.when(~both(row == 1, x == (nx - 2 if d == 0 else 0)))
                            def _():
                                copy = pass_on(m, c, i, d)
                                copy.wait_send() if drain else copy.start()
                            copy = hand(m, c, i, d)
                            copy.wait_send() if drain else copy.start()
                each(2, go)

            @pl.when(~foreign)
            def _():
                @pl.when(needed(p, col, i))
                def _():
                    for d in (0, 1):
                        for copy in (l_own(m, i, d), hand_own(m, i, d)):
                            copy.wait_send() if drain else copy.start()
                if not drain:
                    other = 2 * x + wcore

                    @pl.when(jnp.logical_and(low, needed(p, other, i)))
                    def _():
                        arrived(wpiece(m, other, i), gr.at[m, i, other, 0])
        else:
            def go(e):
                for d in (0, 1):
                    src = (x + nx - hop) % nx if d == 0 else (x + hop) % nx
                    c = 2 * src + e

                    @pl.when(needed(p, c, i))
                    def _():
                        if not drain:
                            arrived(gpiece(m, c, i, d), gr.at[m, i, c, d])
                        if hop < nx - 1:
                            copy = pass_on(m, c, i, d)
                            copy.wait_send() if drain else copy.start()
                        if hop == 1:
                            @pl.when(both(row == 2, x == nx - 1))
                            def _():
                                ref = gpiece(m, c, i, d)
                                copy = remote(ref, ref, inj.at[i, e, d], gr.at[m, i, c, d], device(1, x, 0))
                                copy.wait_send() if drain else copy.start()
                        copy = hand(m, c, i, d)
                        copy.wait_send() if drain else copy.start()
            each(2, go)

    @pl.when(is_g)
    def _():
        def wave(w):
            @pl.when(both(g0, w == nx + 2))
            def _():
                each(TILES, lambda j: b_again(j).start())
            @pl.when(w == 0)
            def _():
                @pl.when(low)
                def _():
                    each(OWN, lambda i: stage(2 * i + 1, 0, False))

                @pl.when(~low)
                def _():
                    each(steps, lambda s: stage(s, 0, False))
            for hop in reversed(range(nx)):
                s = w - hop

                @pl.when(both(s >= 0, s < steps, True if hop else both(low, s != 1, s != 3)))
                def _():
                    stage(s, hop, False)

            for at, first, n in ((0, 0, 1), (1, 1, 2), (nx, 3, TILES - 3)):
                @pl.when(both(last2, w == at))
                def _():
                    each(n, lambda k: b_first(first + k).start())

            @pl.when(jnp.logical_and(low, w >= steps + nx - 1 - OWN))
            def _():
                extra_rows(w - (steps + nx - 1 - OWN))
        each(steps + nx - 1, wave)

        def drain(s):
            for hop in range(nx):
                stage(s, hop, True)
        each(steps, drain)

    count = CHUNKS * TILES

    def code_of(t):
        third = t // 3
        tables = [codes(order) for order in ORDERS]
        word = 0
        for n in range(0, len(tables[0]), 3):
            packed = [sum(v * 512**k for k, v in enumerate(table[n:n + 3])) for table in tables]
            at_row = jnp.where(row == 0, packed[0], jnp.where(row == 1, packed[1], packed[2]))
            word = jnp.where(third == n // 3, at_row, word)
        shift = jnp.where(t % 3 == 0, 1, jnp.where(t % 3 == 1, 512, 512 * 512))
        return word // shift % 512

    @pl.when(is_w)
    def _():
        def fields(code):
            m = code // EXTRA % 2
            return m, jnp.where(m == 1, row, pmain), code % EXTRA // TILES, code % TILES

        def flag(code, bit):
            return code // bit % 2 == 1

        def fetch(code, slot):
            m, p, i, j = fields(code)

            @pl.when(flag(code, LOAD_B))
            def _():
                for q in range(nrow):
                    @pl.when(q <= p)
                    def _():
                        known = jnp.logical_or(jnp.logical_and(forwards, q == fq), both(low, m == 0, q <= row))

                        @pl.when(both(flag(code, FRESH_B), q != row, ~known))
                        def _():
                            arrived(bg.at[q, :, bcols(j)], br.at[q, j])
                        load_b(q, j, slot)

            @pl.when(flag(code, LOAD_L))
            def _():
                load_l(m, p, i, jnp.logical_or(m == 1, ~low), True)

        first = jnp.where(low, 0, OWN * TILES)
        total = OWN * TILES + count

        def step(t, carry):
            code, slot = carry
            m, p, i, j = fields(code)
            for j2, u2 in enumerate(FORWARD_AT):
                @pl.when(both(row == 1, t == u2))
                def _():
                    forward(j2)

            @pl.when(t == first)
            def _():
                fetch(code, slot)

            @pl.when(flag(code, LOAD_B))
            def _():
                for q in range(nrow):
                    @pl.when(q <= p)
                    def _():
                        loaded_b(q, slot)

            @pl.when(flag(code, LOAD_L))
            def _():
                loaded_l(m, p, i)

            following = code_of(t + 1)
            other = jnp.where(flag(following, LOAD_B), 1 - slot, slot)

            @pl.when(t + 1 < total)
            def _():
                fetch(following, other)
            n = t % count
            home = jnp.logical_and(low, m == 0)

            @pl.when(jnp.logical_and(low, t >= count))
            def _():
                sent(ov.at[n], xs.at[n])
            product(m, i, slot, p, n, True)

            @pl.when(home)
            def _():
                x_home(n, i, j).start()

            @pl.when(~home)
            def _():
                x_here(n, i, j).start()
            return following, other
        lax.fori_loop(first, total, step, (code_of(first), 0))

    @pl.when(high_g)
    def _():
        arrived(x_ref, xr)

    @pl.when(is_w)
    def _():
        each(count, lambda t: sent(ov.at[t], xs.at[t]))

    @pl.when(low_g)
    def _():
        each(OWN * TILES, lambda t: sent(ov.at[t], xs.at[t]))

    @pl.when(low_w)
    def _():
        def piece(n):
            c, i = n // OWN, OWN + n % OWN

            @pl.when(jnp.logical_and(needed(row, c, i), c != col))
            def _():
                arrived(wpiece(1, c, i), wr.at[1, i, c])
        each(2 * nx * OWN, piece)

    @pl.when(sends_b)
    def _():
        each(TILES, lambda j: b_first(j).wait_send())

    @pl.when(g0)
    def _():
        each(TILES, lambda j: b_again(j).wait_send())

    @pl.when(forwards)
    def _():
        each(TILES, lambda j: b_forward(j).wait_send())

    def drain(i):
        @pl.when(needed(row, col, i))
        def _():
            @pl.when(~low)
            def _():
                l_to_mirror(i).wait_send()

            @pl.when(is_w)
            def _():
                m = jnp.where(low, 1, 0)
                l_own(m, i, 0).wait_send()
                l_own(m, i, 1).wait_send()

            @pl.when(low_w)
            def _():
                l_to_partner(1, i).wait_send()
    each(CHUNKS, drain)


def finish(nx, l_ref, b_ref, part, bg, lb, x_ref, lv, bv, ov, lvs, bvs, xs):
    rows, width = l_ref.shape
    rc, tw = rows // CHUNKS, b_ref.shape[1] // TILES
    row, col = lax.axis_index("row"), lax.axis_index("col")
    low = row < 2

    def each(n, body):
        lax.fori_loop(0, n, lambda k, carry: (body(k), carry)[1], 0)

    def lrows(i):
        return pl.ds(pl.multiple_of(i * rc, rc), rc)

    def bcols(j):
        return pl.ds(pl.multiple_of(j * tw, tw), tw)

    def needed(c, i):
        return jnp.logical_or(c <= 2 * row, jnp.logical_and(c == 2 * row + 1, i >= CHUNKS // 2))

    def copy_l(i, c, local):
        src = l_ref.at[lrows(i), :] if local else lb.at[1, c, lrows(i), :]
        return pltpu.make_async_copy(src, lv.at[i, :, pl.ds(c * width, width)], lvs.at[i, c])

    def copy_b(j, q, local):
        src = b_ref.at[:, bcols(j)] if local else bg.at[q, :, bcols(j)]
        return pltpu.make_async_copy(src, bv.at[j % SLOTS, pl.ds(q * rows, rows), :], bvs.at[j % SLOTS, q])

    def load_b(j):
        for q in (0, 1):
            @pl.when(q == row)
            def _():
                copy_b(j, q, True).start()

            @pl.when(q < row)
            def _():
                copy_b(j, q, False).start()

    def write(i, j):
        return pltpu.make_async_copy(ov.at[i * TILES + j], x_ref.at[lrows(i), bcols(j)], xs.at[i * TILES + j])

    def read(n):
        return pltpu.make_async_copy(part.at[lrows(n // TILES), bcols(n % TILES)], ov.at[n], xs.at[n])

    def turn(n):
        read(n).wait()
        write(n // TILES, n % TILES).start()

    @pl.when(low)
    def _():
        load_b(0)

        def load_l(i):
            for c in range(4):
                @pl.when(jnp.logical_and(needed(c, i), c == col))
                def _():
                    copy_l(i, c, True).start()

                @pl.when(jnp.logical_and(needed(c, i), c != col))
                def _():
                    copy_l(i, c, False).start()
        each(OWN, lambda i: load_l(OWN + i))
        each(OWN * TILES, lambda n: read(n).start())

        def tile(n):
            i, j = OWN + n % OWN, n // OWN

            @pl.when(i == OWN)
            def _():
                for q in (0, 1):
                    @pl.when(q <= row)
                    def _():
                        copy_b(j, q, True).wait()

                @pl.when(j < TILES - 1)
                def _():
                    load_b(j + 1)

            @pl.when(j == 0)
            def _():
                for c in range(4):
                    @pl.when(needed(c, i))
                    def _():
                        copy_l(i, c, True).wait()
            for p in (0, 1):
                for chunk in range(OWN, CHUNKS):
                    depth = p * rows + (chunk + 1) * rc

                    @pl.when(jnp.logical_and(row == p, i == chunk))
                    def _():
                        ov[i * TILES + j] = jnp.dot(
                            lv[i, :, :depth], bv[j % SLOTS, :depth, :], preferred_element_type=jnp.float32
                        ).astype(ov.dtype)
            write(i, j).start()
        each(OWN * TILES, tile)

    @pl.when(~low)
    def _():
        each(CHUNKS * TILES, lambda n: read(n).start())
    each(jnp.where(low, OWN, CHUNKS) * TILES, turn)
    each(CHUNKS * TILES, lambda n: write(n // TILES, n % TILES).wait())


def solution(mesh):
    nrow, ncol = mesh.shape["row"], mesh.shape["col"]
    spec = P(("batch", "row"), "col")

    def local(l_block, b_block):
        rows, width = l_block.shape
        cols = b_block.shape[1]
        dtype = b_block.dtype
        rc, tw = rows // CHUNKS, cols // TILES
        dma = pltpu.SemaphoreType.DMA
        any_space = pl.BlockSpec(memory_space=pl.ANY)
        part, blocks, strips = pl.pallas_call(
            functools.partial(kernel, nrow, ncol // 2),
            out_shape=(
                jax.ShapeDtypeStruct((rows, cols), dtype),
                jax.ShapeDtypeStruct((nrow, rows, cols), dtype),
                jax.ShapeDtypeStruct((2, ncol, rows, width), dtype),
            ),
            in_specs=[any_space] * 2,
            out_specs=(any_space,) * 3,
            scratch_shapes=[
                pltpu.VMEM((CHUNKS, rc, ncol * width), dtype),
                pltpu.VMEM((SLOTS, nrow * rows, tw), dtype),
                pltpu.VMEM((CHUNKS * TILES, rc, tw), dtype),
                pltpu.VMEM((rc, tw), jnp.float32),
                dma((nrow, TILES)),
                dma((TILES,)),
                dma((TILES,)),
                dma((2, CHUNKS, ncol, 2)),
                dma((2, CHUNKS, ncol)),
                dma((2, CHUNKS, ncol, 2)),
                dma((2, CHUNKS, ncol, 2)),
                dma((CHUNKS,)),
                dma((CHUNKS, 2, 2)),
                dma((CHUNKS, ncol)),
                dma((SLOTS, nrow)),
                dma((CHUNKS * TILES,)),
                dma(()),
            ],
            compiler_params=pltpu.CompilerParams(collective_id=0, has_side_effects=True),
        )(l_block, b_block)
        return pl.pallas_call(
            functools.partial(finish, ncol // 2),
            out_shape=jax.ShapeDtypeStruct((rows, cols), dtype),
            in_specs=[any_space] * 5,
            out_specs=any_space,
            scratch_shapes=[
                pltpu.VMEM((CHUNKS, rc, 4 * width), dtype),
                pltpu.VMEM((SLOTS, 2 * rows, tw), dtype),
                pltpu.VMEM((CHUNKS * TILES, rc, tw), dtype),
                dma((CHUNKS, 4)),
                dma((SLOTS, 2)),
                dma((CHUNKS * TILES,)),
            ],
        )(l_block, b_block, part, blocks, strips)

    return jax.shard_map(local, mesh=mesh, in_specs=(spec, spec), out_specs=spec, check_vma=False)
```

```python
import functools

import jax
import jax.numpy as jnp
from jax import lax
from jax.experimental import pallas as pl
from jax.experimental.pallas import tpu as pltpu
from jax.sharding import PartitionSpec as P

MESH = pl.DeviceIdType.MESH
CHUNKS = 4
TILES = 8
SLOTS = 2

OWN = CHUNKS // 2
REST = " 24 23 22 21 20 05 15 25 06 16 26 07 17 27 37 36 35 34 33 32 31 30"
ORDERS = (
    " ".join(f"E{i}{j}" for j in range(TILES) for i in range(CHUNKS)) + " 00 01 02 10 11 12 03 13 04 14" + REST,
    " ".join(f"E0{j}" for j in range(TILES)) + " 00 01 10 11 02 12 "
    + " ".join(f"E1{j}" for j in range(TILES))
    + " 03 13 23 22 21 20 04 14 24 05 15 25 06 16 26 07 17 27 37 36 35 34 33 32 31 30",
    "00 01 02 03 10 11 12 13 20 21 22 23 04 14 24 30 31 32 33 34 05 15 25 35 06 16 26 36 07 17 27 37",
)
SPAN = 2 * CHUNKS * TILES
FORWARD_AT = (16, 20, 27, 37, 43, 46, 49, 52)
EXTRA, LOAD_B, FRESH_B, LOAD_L = 32, 64, 128, 256


def codes(order):
    tiles = [(len(t) - 2, int(t[-2]), int(t[-1])) for t in order.split()]
    out = []
    for n, (extra, i, j) in enumerate(tiles):
        code = i * TILES + j + EXTRA * extra
        if n == 0 or tiles[n - 1][2] != j or tiles[n - 1][0] != extra:
            code += LOAD_B
        if (extra, j) not in [(e, b) for e, _, b in tiles[:n]]:
            code += FRESH_B
        if (extra, i) not in [(e, a) for e, a, _ in tiles[:n]]:
            code += LOAD_L
        out.append(code)
    return [0] * (SPAN - len(out)) + out


def kernel(nrow, nx, l_ref, b_ref, x_ref, bg, lb, lv, bv, ov, acc,
           br, bs, bs2, gr, wr, ls, ps, ly, inj, lvs, bvs, xs, xr):
    rows, width = l_ref.shape
    cols = b_ref.shape[1]
    rc, half, tw = rows // CHUNKS, rows // CHUNKS // 2, cols // TILES

    row, col = lax.axis_index("row"), lax.axis_index("col")
    x, core = col // 2, col % 2
    right, left = (x + 1) % nx, (x + nx - 1) % nx
    up, down = (row + nrow - 1) % nrow, (row + 1) % nrow
    low = row < 2
    mirror = nrow - 1 - row
    wcore = jnp.where(low, 1, 0)
    gcore = 1 - wcore
    pmain = jnp.where(low, mirror, row)
    is_w, is_g = core == wcore, core == gcore
    low_w, low_g = jnp.logical_and(low, is_w), jnp.logical_and(low, is_g)
    high_w, high_g = jnp.logical_and(~low, is_w), jnp.logical_and(~low, is_g)

    def both(*conditions):
        return functools.reduce(jnp.logical_and, conditions)

    def needed(p, c, i):
        return jnp.logical_or(c <= 2 * p, jnp.logical_and(c == 2 * p + 1, i >= CHUNKS // 2))

    def device(r, xx, k):
        return {"row": r, "col": xx * 2 + k}

    partner = device(row, x, 1 - core)

    def remote(src, dst, send, recv, to):
        return pltpu.make_async_remote_copy(
            src_ref=src, dst_ref=dst, send_sem=send, recv_sem=recv, device_id=to, device_id_type=MESH)

    def arrived(ref, sem):
        pltpu.make_async_copy(ref, ref, sem).wait()

    def sent(ref, sem):
        pltpu.make_async_copy(ref, ref, sem).wait()

    def each(n, body):
        lax.fori_loop(0, n, lambda k, carry: (body(k), carry)[1], 0)

    barrier = pltpu.get_barrier_semaphore()
    peers = [partner] + [device(r, xx, k) for k in (0, 1)
                         for r, xx in ((row, right), (row, left), (up, x), (down, x))]
    for peer in peers:
        pl.semaphore_signal(barrier, inc=1, device_id=peer, device_id_type=MESH)
    pl.semaphore_wait(barrier, len(peers))

    def lrows(i):
        return pl.ds(pl.multiple_of(i * rc, rc), rc)

    def lhalf(i, d):
        return pl.ds(pl.multiple_of(i * rc + d * half, half), half)

    def bcols(j):
        return pl.ds(pl.multiple_of(j * tw, tw), tw)

    def gpiece(m, c, i, d):
        return lb.at[m, c, lhalf(i, d), :]

    def wpiece(m, c, i):
        return lb.at[m, c, lrows(i), :]

    def l_to_mirror(i):
        return remote(l_ref.at[lrows(i), :], wpiece(0, col, i), ly.at[i], gr.at[0, i, col, 0], device(mirror, x, 0))

    def l_own(m, i, d):
        return remote(l_ref.at[lhalf(i, d), :], gpiece(m, col, i, d), ls.at[m, i, col, d], gr.at[m, i, col, d],
                      device(row, right if d == 0 else left, gcore))

    def l_to_partner(m, i):
        return remote(l_ref.at[lrows(i), :], wpiece(m, col, i), ly.at[i], gr.at[m, i, col, 0], partner)

    first_row = jnp.where(core == 0,
                          jnp.where(row == 1, 2, 3),
                          jnp.where(row == 1, 0, jnp.where(row == 3, 0, 1)))

    def b_first(j):
        return remote(b_ref.at[:, bcols(j)], bg.at[row, :, bcols(j)], bs.at[j], br.at[row, j], device(first_row, x, core))

    def b_again(j):
        return remote(b_ref.at[:, bcols(j)], bg.at[0, :, bcols(j)], bs2.at[j], br.at[0, j], device(1, x, 0))

    fq = jnp.where(row == 3, 0, jnp.where(row == 2, 1, 2))
    ft = jnp.where(row == 3, 2, jnp.where(row == 2, 3, 0))
    forwards = jnp.logical_and(is_w, row > 0)

    def b_forward(j):
        ref = bg.at[fq, :, bcols(j)]
        return remote(ref, ref, bs2.at[j], br.at[fq, j], device(ft, x, core))

    def forward(j):
        arrived(bg.at[fq, :, bcols(j)], br.at[fq, j])
        b_forward(j).start()

    sends_b = ~both(row == 3, core == 0)
    g0 = both(row == 0, core == 0)
    w2 = both(row == 2, core == 0)
    last2 = both(row == 2, core == 1, x == nx - 1)

    def start_b(*js):
        for j in js:
            b_first(j).start()

    def start_l(i):
        @pl.when(needed(row, col, i))
        def _():
            l_to_mirror(i).start()

    @pl.when(is_w)
    def _():
        def go(i):
            @pl.when(needed(row, col, i))
            def _():
                m = jnp.where(low, 1, 0)
                l_own(m, i, 0).start()
                l_own(m, i, 1).start()

                @pl.when(low)
                def _():
                    l_to_partner(1, i).start()
        each(CHUNKS, go)

    @pl.when(high_w)
    def _():
        each(jnp.where(w2, OWN, CHUNKS), start_l)

        def go(j):
            @pl.when(w2)
            def _():
                b_first(j).start()
            forward(j)
            for j2, i in ((4, 2), (7, 3)):
                @pl.when(jnp.logical_and(w2, j == j2))
                def _():
                    start_l(i)
        each(TILES, go)

    @pl.when(both(high_g, row == 3))
    def _():
        each(CHUNKS, start_l)
        each(TILES, lambda j: b_first(j).start())

    @pl.when(both(high_g, row == 2, ~last2))
    def _():
        start_l(0)
        start_l(1)
        start_b(0, 1)
        start_l(2)
        start_b(2)
        start_l(3)
        start_b(*range(3, TILES))

    @pl.when(low)
    def _():
        each(TILES, lambda j: b_first(j).start())

    def place(m, i):
        own_a = jnp.where(row == 0, CHUNKS - 1 - i // 2, CHUNKS - 1)
        own_k = i % 2 * (2 * rows)
        return jnp.where(m == 0, i, own_a), jnp.where(m == 0, 0, own_k)

    def product(m, i, slot, p, t, deep):
        a, k0 = place(m, i)

        def dot(first, depth):
            lhs = lv[a, :, pl.ds(pl.multiple_of(k0 + first, rows), depth)]
            return jnp.dot(lhs, bv[slot, pl.ds(first, depth), :], preferred_element_type=jnp.float32)

        if deep:
            @pl.when(p >= 2)
            def _():
                acc[...] = dot(0, 2 * rows)
        for odd in (0, 1):
            for chunk in range(CHUNKS):
                depth = odd * rows + (chunk + 1) * rc

                @pl.when(both(p % 2 == odd, i == chunk))
                def _():
                    if deep:
                        last = dot(pl.multiple_of(p // 2 * (2 * rows), rows), depth)
                        ov[t] = (jnp.where(p >= 2, acc[...], 0.0) + last).astype(ov.dtype)
                    else:
                        ov[t] = dot(0, depth).astype(ov.dtype)

    def copy_l(m, i, c, local):
        a, k0 = place(m, i)
        src = l_ref.at[lrows(i), :] if local else wpiece(m, c, i)
        to = lv.at[a, :, pl.ds(pl.multiple_of(k0 + c * width, width), width)]
        return pltpu.make_async_copy(src, to, lvs.at[i, c])

    def load_l(m, p, i, own, wait):
        def start(c):
            @pl.when(needed(p, c, i))
            def _():
                mine = jnp.logical_and(own, c == col)

                @pl.when(mine)
                def _():
                    copy_l(m, i, c, True).start()

                @pl.when(~mine)
                def _():
                    if wait:
                        arrived(wpiece(m, c, i), wr.at[m, i, c])
                    copy_l(m, i, c, False).start()
        each(2 * nx, start)

    def loaded_l(m, p, i):
        def finish(c):
            @pl.when(needed(p, c, i))
            def _():
                copy_l(m, i, c, True).wait()
        each(2 * nx, finish)

    def load_b(q, j, slot):
        def copy(local):
            src = b_ref.at[:, bcols(j)] if local else bg.at[q, :, bcols(j)]
            to = bv.at[slot, pl.ds(q * rows, rows), :]
            return pltpu.make_async_copy(src, to, bvs.at[slot, q])

        @pl.when(q == row)
        def _():
            copy(True).start()

        @pl.when(q != row)
        def _():
            copy(False).start()

    def loaded_b(q, slot):
        pltpu.make_async_copy(b_ref.at[:, bcols(0)], bv.at[slot, pl.ds(q * rows, rows), :], bvs.at[slot, q]).wait()

    def x_home(t, i, j):
        return remote(ov.at[t], x_ref.at[lrows(i), bcols(j)], xs.at[t], xr, device(mirror, x, core))

    def x_here(t, i, j):
        return pltpu.make_async_copy(ov.at[t], x_ref.at[lrows(i), bcols(j)], xs.at[t])

    def extra_columns(j):
        slot = j % SLOTS
        load_b(0, j, slot)
        loaded_b(0, slot)

        def tile(i):
            product(1, i, slot, row, i * TILES + j, False)
            x_here(i * TILES + j, i, j).start()
        each(CHUNKS, tile)

    def extra_rows(i):
        def start(j):
            for q in (0, 1):
                @pl.when(q <= row)
                def _():
                    @pl.when(jnp.logical_and(q != row, i == 0))
                    def _():
                        arrived(bg.at[q, :, bcols(j)], br.at[q, j])
                    load_b(q, j, j % SLOTS)

        load_l(1, row, i, True, False)
        start(0)
        loaded_l(1, row, i)

        def tile(j):
            for q in (0, 1):
                @pl.when(q <= row)
                def _():
                    loaded_b(q, j % SLOTS)

            @pl.when(j < TILES - 1)
            def _():
                start(j + 1)
            product(1, i, j % SLOTS, row, i * TILES + j, False)
            x_here(i * TILES + j, i, j).start()
        each(TILES, tile)

    def hand(m, c, i, d):
        ref = gpiece(m, c, i, d)
        return remote(ref, ref, ps.at[m, i, c, d], wr.at[m, i, c], partner)

    def hand_own(m, i, d):
        return remote(l_ref.at[lhalf(i, d), :], gpiece(m, col, i, d), ps.at[m, i, col, d], wr.at[m, i, col], partner)

    def pass_on(m, c, i, d):
        ref = gpiece(m, c, i, d)
        return remote(ref, ref, ls.at[m, i, c, d], gr.at[m, i, c, d], device(row, right if d == 0 else left, gcore))

    steps = jnp.where(low, 2 * CHUNKS, CHUNKS)

    def stage(s, hop, drain):
        m = jnp.where(row == 0, 1 - s // CHUNKS, jnp.where(row == 1, s % 2, 0))
        i = jnp.where(row == 1, s // 2, s % CHUNKS)
        p = jnp.where(m == 0, pmain, row)
        if hop == 0:
            foreign = jnp.logical_and(low, m == 0)

            @pl.when(foreign)
            def _():
                def go(e):
                    c = 2 * x + e

                    @pl.when(needed(p, c, i))
                    def _():
                        if not drain:
                            arrived(wpiece(m, c, i), gr.at[m, i, c, 0])
                        for d in (0, 1):
                            @pl.when(~both(row == 1, x == (nx - 2 if d == 0 else 0)))
                            def _():
                                copy = pass_on(m, c, i, d)
                                copy.wait_send() if drain else copy.start()
                            copy = hand(m, c, i, d)
                            copy.wait_send() if drain else copy.start()
                each(2, go)

            @pl.when(~foreign)
            def _():
                @pl.when(needed(p, col, i))
                def _():
                    for d in (0, 1):
                        for copy in (l_own(m, i, d), hand_own(m, i, d)):
                            copy.wait_send() if drain else copy.start()
                if not drain:
                    other = 2 * x + wcore

                    @pl.when(jnp.logical_and(low, needed(p, other, i)))
                    def _():
                        arrived(wpiece(m, other, i), gr.at[m, i, other, 0])
        else:
            def go(e):
                for d in (0, 1):
                    src = (x + nx - hop) % nx if d == 0 else (x + hop) % nx
                    c = 2 * src + e

                    @pl.when(needed(p, c, i))
                    def _():
                        if not drain:
                            arrived(gpiece(m, c, i, d), gr.at[m, i, c, d])
                        if hop < nx - 1:
                            copy = pass_on(m, c, i, d)
                            copy.wait_send() if drain else copy.start()
                        if hop == 1:
                            @pl.when(both(row == 2, x == nx - 1))
                            def _():
                                ref = gpiece(m, c, i, d)
                                copy = remote(ref, ref, inj.at[i, e, d], gr.at[m, i, c, d], device(1, x, 0))
                                copy.wait_send() if drain else copy.start()
                        copy = hand(m, c, i, d)
                        copy.wait_send() if drain else copy.start()
            each(2, go)

    @pl.when(is_g)
    def _():
        def wave(w):
            @pl.when(both(g0, w == nx + 3))
            def _():
                each(TILES, lambda j: b_again(j).start())
            @pl.when(w == 0)
            def _():
                @pl.when(row == 1)
                def _():
                    each(OWN, lambda i: stage(2 * i + 1, 0, False))

                @pl.when(row != 1)
                def _():
                    each(CHUNKS, lambda s: stage(s, 0, False))
            for hop in reversed(range(nx)):
                s = w - hop

                @pl.when(both(s >= 0, s < steps, True if hop else jnp.where(row == 1, both(s != 1, s != 3), s >= CHUNKS)))
                def _():
                    stage(s, hop, False)

            for at, first, n in ((0, 0, 1), (1, 1, 2), (nx, 3, TILES - 3)):
                @pl.when(both(last2, w == at))
                def _():
                    each(n, lambda k: b_first(first + k).start())

            k = w - (steps + nx - 4)

            @pl.when(both(row == 1, k >= 0, k < OWN))
            def _():
                extra_rows(k)
        each(steps + nx - 1, wave)

        @pl.when(row == 0)
        def _():
            each(CHUNKS, lambda i: load_l(1, row, i, True, False))
            each(CHUNKS, lambda i: loaded_l(1, row, i))
            each(TILES, extra_columns)

        def drain(s):
            for hop in range(nx):
                stage(s, hop, True)
        each(steps, drain)

    count = CHUNKS * TILES

    def code_of(t):
        third = t // 3
        tables = [codes(order) for order in ORDERS]
        word = 0
        for n in range(0, len(tables[0]), 3):
            packed = [sum(v * 512**k for k, v in enumerate(table[n:n + 3])) for table in tables]
            at_row = jnp.where(row == 0, packed[0], jnp.where(row == 1, packed[1], packed[2]))
            word = jnp.where(third == n // 3, at_row, word)
        shift = jnp.where(t % 3 == 0, 1, jnp.where(t % 3 == 1, 512, 512 * 512))
        return word // shift % 512

    @pl.when(is_w)
    def _():
        def fields(code):
            m = code // EXTRA % 2
            return m, jnp.where(m == 1, row, pmain), code % EXTRA // TILES, code % TILES

        def flag(code, bit):
            return code // bit % 2 == 1

        def fetch(code, slot):
            m, p, i, j = fields(code)

            @pl.when(flag(code, LOAD_B))
            def _():
                for q in range(nrow):
                    @pl.when(q <= p)
                    def _():
                        known = jnp.logical_or(jnp.logical_and(forwards, q == fq), both(low, m == 0, q <= row))

                        @pl.when(both(flag(code, FRESH_B), q != row, ~known))
                        def _():
                            arrived(bg.at[q, :, bcols(j)], br.at[q, j])
                        load_b(q, j, slot)

            @pl.when(flag(code, LOAD_L))
            def _():
                load_l(m, p, i, jnp.logical_or(m == 1, ~low), True)

        first = jnp.where(row == 0, 0, jnp.where(row == 1, OWN * TILES, count))

        def step(t, carry):
            code, slot = carry
            m, p, i, j = fields(code)
            for j2, u2 in enumerate(FORWARD_AT):
                @pl.when(both(row == 1, t == u2))
                def _():
                    forward(j2)

            @pl.when(t == first)
            def _():
                fetch(code, slot)

            @pl.when(flag(code, LOAD_B))
            def _():
                for q in range(nrow):
                    @pl.when(q <= p)
                    def _():
                        loaded_b(q, slot)

            @pl.when(flag(code, LOAD_L))
            def _():
                loaded_l(m, p, i)

            following = code_of(t + 1)
            other = jnp.where(flag(following, LOAD_B), 1 - slot, slot)

            @pl.when(t + 1 < SPAN)
            def _():
                fetch(following, other)
            n = t % count
            home = jnp.logical_and(low, m == 0)

            @pl.when(t >= first + count)
            def _():
                sent(ov.at[n], xs.at[n])
            product(m, i, slot, p, n, True)

            @pl.when(home)
            def _():
                x_home(n, i, j).start()

            @pl.when(~home)
            def _():
                x_here(n, i, j).start()
            return following, other
        lax.fori_loop(first, SPAN, step, (code_of(first), 0))

    @pl.when(high_g)
    def _():
        arrived(x_ref, xr)

    @pl.when(is_w)
    def _():
        each(count, lambda t: sent(ov.at[t], xs.at[t]))

    @pl.when(low_g)
    def _():
        each(jnp.where(row == 0, CHUNKS, OWN) * TILES, lambda t: sent(ov.at[t], xs.at[t]))

    @pl.when(jnp.logical_and(low_w, row == 1))
    def _():
        def piece(n):
            c, i = n // OWN, OWN + n % OWN

            @pl.when(jnp.logical_and(needed(row, c, i), c != col))
            def _():
                arrived(wpiece(1, c, i), wr.at[1, i, c])
        each(2 * nx * OWN, piece)

    @pl.when(sends_b)
    def _():
        each(TILES, lambda j: b_first(j).wait_send())

    @pl.when(g0)
    def _():
        each(TILES, lambda j: b_again(j).wait_send())

    @pl.when(forwards)
    def _():
        each(TILES, lambda j: b_forward(j).wait_send())

    def drain(i):
        @pl.when(needed(row, col, i))
        def _():
            @pl.when(~low)
            def _():
                l_to_mirror(i).wait_send()

            @pl.when(is_w)
            def _():
                m = jnp.where(low, 1, 0)
                l_own(m, i, 0).wait_send()
                l_own(m, i, 1).wait_send()

            @pl.when(low_w)
            def _():
                l_to_partner(1, i).wait_send()
    each(CHUNKS, drain)


def finish(nx, l_ref, b_ref, part, bg, lb, x_ref, lv, bv, ov, lvs, bvs, xs):
    rows, width = l_ref.shape
    rc, tw = rows // CHUNKS, b_ref.shape[1] // TILES
    row, col = lax.axis_index("row"), lax.axis_index("col")
    low = row == 1
    done = jnp.where(low, OWN, CHUNKS)
    left = CHUNKS - done

    def each(n, body):
        lax.fori_loop(0, n, lambda k, carry: (body(k), carry)[1], 0)

    def lrows(i):
        return pl.ds(pl.multiple_of(i * rc, rc), rc)

    def bcols(j):
        return pl.ds(pl.multiple_of(j * tw, tw), tw)

    def needed(c, i):
        return jnp.logical_or(c <= 2 * row, jnp.logical_and(c == 2 * row + 1, i >= CHUNKS // 2))

    def copy_l(i, c, local):
        src = l_ref.at[lrows(i), :] if local else lb.at[1, c, lrows(i), :]
        return pltpu.make_async_copy(src, lv.at[i, :, pl.ds(c * width, width)], lvs.at[i, c])

    def copy_b(j, q, local):
        src = b_ref.at[:, bcols(j)] if local else bg.at[q, :, bcols(j)]
        return pltpu.make_async_copy(src, bv.at[j % SLOTS, pl.ds(q * rows, rows), :], bvs.at[j % SLOTS, q])

    def load_b(j):
        for q in (0, 1):
            @pl.when(q == row)
            def _():
                copy_b(j, q, True).start()

            @pl.when(q < row)
            def _():
                copy_b(j, q, False).start()

    def write(i, j):
        return pltpu.make_async_copy(ov.at[i * TILES + j], x_ref.at[lrows(i), bcols(j)], xs.at[i * TILES + j])

    def read(n):
        return pltpu.make_async_copy(part.at[lrows(n // TILES), bcols(n % TILES)], ov.at[n], xs.at[n])

    def turn(n):
        read(n).wait()
        write(n // TILES, n % TILES).start()

    @pl.when(low)
    def _():
        load_b(0)

        def load_l(i):
            for c in range(4):
                @pl.when(jnp.logical_and(needed(c, i), c == col))
                def _():
                    copy_l(i, c, True).start()

                @pl.when(jnp.logical_and(needed(c, i), c != col))
                def _():
                    copy_l(i, c, False).start()
        each(left, lambda i: load_l(done + i))
        each(done * TILES, lambda n: read(n).start())

        def tile(n):
            i, j = done + n % left, n // left

            @pl.when(i == done)
            def _():
                for q in (0, 1):
                    @pl.when(q <= row)
                    def _():
                        copy_b(j, q, True).wait()

                @pl.when(j < TILES - 1)
                def _():
                    load_b(j + 1)

            @pl.when(j == 0)
            def _():
                for c in range(4):
                    @pl.when(needed(c, i))
                    def _():
                        copy_l(i, c, True).wait()
            for chunk in range(OWN, CHUNKS):
                depth = rows + (chunk + 1) * rc

                @pl.when(i == chunk)
                def _():
                    ov[i * TILES + j] = jnp.dot(
                        lv[i, :, :depth], bv[j % SLOTS, :depth, :], preferred_element_type=jnp.float32
                    ).astype(ov.dtype)
            write(i, j).start()
        each(left * TILES, tile)

    @pl.when(~low)
    def _():
        each(CHUNKS * TILES, lambda n: read(n).start())
    each(done * TILES, turn)
    each(CHUNKS * TILES, lambda n: write(n // TILES, n % TILES).wait())


def solution(mesh):
    nrow, ncol = mesh.shape["row"], mesh.shape["col"]
    spec = P(("batch", "row"), "col")

    def local(l_block, b_block):
        rows, width = l_block.shape
        cols = b_block.shape[1]
        dtype = b_block.dtype
        rc, tw = rows // CHUNKS, cols // TILES
        dma = pltpu.SemaphoreType.DMA
        any_space = pl.BlockSpec(memory_space=pl.ANY)
        part, blocks, strips = pl.pallas_call(
            functools.partial(kernel, nrow, ncol // 2),
            out_shape=(
                jax.ShapeDtypeStruct((rows, cols), dtype),
                jax.ShapeDtypeStruct((nrow, rows, cols), dtype),
                jax.ShapeDtypeStruct((2, ncol, rows, width), dtype),
            ),
            in_specs=[any_space] * 2,
            out_specs=(any_space,) * 3,
            scratch_shapes=[
                pltpu.VMEM((CHUNKS, rc, ncol * width), dtype),
                pltpu.VMEM((SLOTS, nrow * rows, tw), dtype),
                pltpu.VMEM((CHUNKS * TILES, rc, tw), dtype),
                pltpu.VMEM((rc, tw), jnp.float32),
                dma((nrow, TILES)),
                dma((TILES,)),
                dma((TILES,)),
                dma((2, CHUNKS, ncol, 2)),
                dma((2, CHUNKS, ncol)),
                dma((2, CHUNKS, ncol, 2)),
                dma((2, CHUNKS, ncol, 2)),
                dma((CHUNKS,)),
                dma((CHUNKS, 2, 2)),
                dma((CHUNKS, ncol)),
                dma((SLOTS, nrow)),
                dma((CHUNKS * TILES,)),
                dma(()),
            ],
            compiler_params=pltpu.CompilerParams(collective_id=0, has_side_effects=True),
        )(l_block, b_block)
        return pl.pallas_call(
            functools.partial(finish, ncol // 2),
            out_shape=jax.ShapeDtypeStruct((rows, cols), dtype),
            in_specs=[any_space] * 5,
            out_specs=any_space,
            scratch_shapes=[
                pltpu.VMEM((CHUNKS, rc, 4 * width), dtype),
                pltpu.VMEM((SLOTS, 2 * rows, tw), dtype),
                pltpu.VMEM((CHUNKS * TILES, rc, tw), dtype),
                dma((CHUNKS, 4)),
                dma((SLOTS, 2)),
                dma((CHUNKS * TILES,)),
            ],
        )(l_block, b_block, part, blocks, strips)

    return jax.shard_map(local, mesh=mesh, in_specs=(spec, spec), out_specs=spec, check_vma=False)
```
